32 devices in a mesh: mem: 4 (over x, core), ty: 2 (over y), tx: 4 (over z).
Axes of the slice: x: 2, y: 2, z: 4, core: 2. Of those that a mesh axis runs over, the one named last changes fastest.
Arguments:
- pressure: float32 [8, 50, 64, 512], P('mem', None, 'ty', 'tx'), may hold values from -6 to 6
- east_wind: float32 [8, 50, 64, 512], P('mem', None, 'ty', 'tx'), may hold values from -6 to 6
- north_wind: float32 [8, 50, 64, 512], P('mem', None, 'ty', 'tx'), may hold values from -6 to 6
- vertical_wind: float32 [8, 49, 64, 512], P('mem', None, 'ty', 'tx'), may hold values from -6 to 6
- sound_squared: float32 [50, 64, 512], P(None, 'ty', 'tx'), may hold values from 0.5 to 2
- thickness: float32 [50], replicated, may hold values from 0.05 to 0.5
- owner_map: int32 [8], replicated, may hold values from 0 to 7, each once
Outputs:
- analysis: float32 [2, 4, 6, 32, 128], P('ty', 'tx', None, 'mem')
The draws below stay inside these ranges and needn't reach their ends.
Inputs may be any that keep to these rules, and one draw needn't show every extreme that they name: `owner_map`: every tile index appears exactly once.
All inputs are finite; a program needn't handle non-finite values.
Results may differ from the reference program's by a relative error of at most 0.0001.
Values sent between devices are 32-bit elements; how exact they have to be, the bound alone decides.
A program may use at most 128 MiB of HBM per device.

```python
import math
import jax
import jax.numpy as jnp
from jax import lax

CY = 32
CX = 128
NZ = 50
SUBSTEPS = 2
MEMBERS = 8
NY = 64
NX = 512
WLEVELS = 49
TILES = 8
N_TY = 2
N_TX = 4


def levels(stream_key, dims, split, smallest, largest):
    def one(axis_at, parts):
        draws = jax.random.uniform(jax.random.fold_in(jax.random.fold_in(stream_key, 6), axis_at), (parts,), jnp.float32, smallest / len(split), largest / len(split))
        return jnp.repeat(jnp.exp(draws), dims[axis_at] // parts).reshape((-1,) + (1,) * (len(dims) - axis_at - 1))

    loudness = one(*split[0])
    for cut in split[1:]:
        loudness = loudness * one(*cut)
    return loudness


def noise(rng, shape, scale, most, pieces=(), held_as=jnp.bfloat16):
    array = jax.random.normal(rng, shape, jnp.float32) * scale
    if len(pieces) > 0:
        array = levels(rng, shape, pieces, -0.22, 0.18) * array
    return jnp.clip(array, min=-most, max=most).astype(held_as)


def setup_inputs(seed: int = 0) -> dict:
    key_list = jax.random.split(jax.random.key(seed), 8)
    return {
        "pressure": noise(key_list[0], (MEMBERS, NZ, NY, NX), 1.0, 6.0, ((0, 4), (2, 2), (3, 4)), jnp.float32),
        "east_wind": noise(key_list[1], (MEMBERS, NZ, NY, NX), 1.0, 6.0, ((0, 4), (2, 2), (3, 4)), jnp.float32),
        "north_wind": noise(key_list[2], (MEMBERS, NZ, NY, NX), 1.0, 6.0, ((0, 4), (2, 2), (3, 4)), jnp.float32),
        "vertical_wind": noise(key_list[3], (MEMBERS, WLEVELS, NY, NX), 1.0, 6.0, ((0, 4), (2, 2), (3, 4)), jnp.float32),
        "sound_squared": jnp.clip(jnp.exp(math.log(2.0) - 1.3862944 * jax.random.uniform(key_list[4], (NZ, NY, NX), jnp.float32) ** levels(key_list[4], (NZ, NY, NX), ((1, 2), (2, 4)), -0.2, 0.2)), 0.5, 2.0),
        "thickness": jnp.clip(jnp.exp(jax.random.uniform(key_list[5], (NZ,), jnp.float32, math.log(0.05), math.log(0.5))), 0.05, 0.5),
        "owner_map": jax.random.permutation(key_list[6], TILES).astype(jnp.int32),
    }


horiz_ratio = 0.35
vert_ratio = 1.5


def column_solve(coeff, rhs_list):
    count = len(rhs_list)
    factors = []
    values = []
    pivot = 1.0 + coeff[1] + coeff[0]
    values.append(rhs_list[0] / pivot)
    factors.append(-coeff[1] / pivot)
    for position in range(1, count):
        pivot = (1.0 + coeff[position + 1] + coeff[position]) + coeff[position] * factors[position - 1]
        values.append((rhs_list[position] + coeff[position] * values[position - 1]) / pivot)
        factors.append(-coeff[position + 1] / pivot)
    solved = [values[count - 1]]
    for position in range(count - 2, -1, -1):
        solved.insert(0, values[position] - factors[position] * solved[0])
    return solved


def member_run(pressure, east_wind, north_wind, vertical_wind, sound_squared, thickness):
    coeff_field = vert_ratio * vert_ratio * sound_squared
    coeff = [coeff_field[level] for level in range(NZ)]
    for substep in range(SUBSTEPS):
        east_wind = east_wind - horiz_ratio * (pressure - jnp.roll(pressure, 1, axis=2))
        north_wind = north_wind - horiz_ratio * (pressure - jnp.roll(pressure, 1, axis=1))
        divergence = (jnp.roll(east_wind, -1, axis=2) - east_wind) + (jnp.roll(north_wind, -1, axis=1) - north_wind)
        partial_value = pressure - horiz_ratio * sound_squared * divergence
        rhs_list = [vertical_wind[level] - vert_ratio * (partial_value[level + 1] - partial_value[level]) for level in range(NZ - 1)]
        vertical_wind = jnp.stack(column_solve(coeff, rhs_list), axis=0)
        zero_layer = jnp.zeros_like(partial_value[:1])
        padded = jnp.concatenate([zero_layer, vertical_wind, zero_layer], axis=0)
        pressure = partial_value - vert_ratio * sound_squared * (padded[1:] - padded[:-1])
    mass = jnp.einsum('k,kyx->yx', thickness, pressure, precision=lax.Precision.HIGHEST)
    east_total = jnp.einsum('k,kyx->yx', thickness, east_wind, precision=lax.Precision.HIGHEST)
    north_total = jnp.einsum('k,kyx->yx', thickness, north_wind, precision=lax.Precision.HIGHEST)
    return jnp.stack([mass, east_total, north_total], axis=0)


def reference(pressure, east_wind, north_wind, vertical_wind, sound_squared, thickness, owner_map):
    def one_member(fields):
        return member_run(fields[0], fields[1], fields[2], fields[3], sound_squared, thickness)

    integrals = lax.map(one_member, (pressure, east_wind, north_wind, vertical_wind))
    mean = jnp.sum(integrals, axis=0) / MEMBERS
    variance = jnp.sum((integrals - mean) ** 2, axis=0) / (MEMBERS - 1)
    stats = jnp.concatenate([mean, variance], axis=0)
    tiled = stats.reshape(6, N_TY, CY, N_TX, CX).transpose(1, 3, 0, 2, 4).reshape(N_TY * N_TX, 6, CY, CX)
    placed = jnp.zeros_like(tiled).at[owner_map.astype(jnp.int32)].set(tiled)
    return placed.reshape(N_TY, N_TX, 6, CY, CX)
```

```python
import functools

import jax
import jax.numpy as jnp
from jax import lax
from jax.experimental import pallas as pl
from jax.experimental.pallas import tpu as pltpu
from jax.sharding import PartitionSpec as P

SUBSTEPS = 2
MESH = pl.DeviceIdType.MESH

horiz_ratio = 0.35
vert_ratio = 1.5


def unrolled(count, body, carry, most=7):
    width = max(d for d in range(1, most + 1) if count % d == 0)

    def block(i, c):
        for j in range(width):
            c = body(i * width + j, c)
        return c

    return lax.fori_loop(0, count // width, block, carry)


def kernel(
    sizes,
    p_hbm, u_hbm, v_hbm, w_hbm, s_hbm, thick, owner,
    out,
    p, u, v, w, s, inv, g,
    csend, crecv, rsend, rrecv, ueast, vnorth,
    integ, gath, everyone,
    load_sem, cs_sem, cr_sem, rs_sem, rr_sem, ms_sem, mr_sem, as_sem, ar_sem,
):
    n_mem, n_ty, n_tx = sizes
    own, levels, rows, cols = p.shape
    quarter = rows // n_mem
    tiles = n_ty * n_tx
    mem, ty, tx = lax.axis_index("mem"), lax.axis_index("ty"), lax.axis_index("tx")
    me = ty * n_tx + tx
    east, west = {"tx": lax.rem(tx + 1, n_tx)}, {"tx": lax.rem(tx + n_tx - 1, n_tx)}
    north, south = {"ty": lax.rem(ty + 1, n_ty)}, {"ty": lax.rem(ty + n_ty - 1, n_ty)}
    lane = lax.broadcasted_iota(jnp.int32, (rows, cols), 1)
    row = lax.broadcasted_iota(jnp.int32, (rows, cols), 0)
    zero = jnp.zeros((rows, cols), jnp.float32)

    def load(src, dst, sem):
        copy = pltpu.make_async_copy(src, dst, load_sem.at[sem])
        copy.start()
        return copy

    loads = {}
    for m in range(own):
        for i, (name, src, dst) in enumerate((("p", p_hbm, p), ("u", u_hbm, u), ("v", v_hbm, v))):
            loads[name, m] = load(src.at[m], dst.at[m], 4 * m + i)
        if m == 0:
            loads["s"] = load(s_hbm, s, 4 * own)
    for m in range(own):
        loads["w", m] = load(w_hbm.at[m], w.at[m], 4 * m + 3)

    barrier = pltpu.get_barrier_semaphore()

    def tile_id(i):
        other = lax.rem(me + i, tiles)
        return other, {"ty": lax.div(other, n_tx), "tx": lax.rem(other, n_tx)}

    def mem_id(i):
        other = lax.rem(mem + i, n_mem)
        return other, {"mem": other}

    for i in range(1, tiles):
        pl.semaphore_signal(barrier, inc=1, device_id=tile_id(i)[1], device_id_type=MESH)
    for i in range(1, n_mem):
        pl.semaphore_signal(barrier, inc=1, device_id=mem_id(i)[1], device_id_type=MESH)

    def remote(src, dst, ssem, rsem, where):
        return pltpu.make_async_remote_copy(
            src_ref=src, dst_ref=dst, send_sem=ssem, recv_sem=rsem, device_id=where, device_id_type=MESH
        )

    def halo_copies(sub, m):
        kinds = ((0, east, north), (1, west, south), (2, west, south))
        copies = []
        for kind, across, along in kinds if sub == 0 else kinds[:2]:
            copies.append(remote(
                rsend.at[sub, m, kind], rrecv.at[sub, m, kind],
                rs_sem.at[sub, m, kind], rr_sem.at[sub, m, kind], along))
            copies.append(remote(
                csend.at[sub, m, kind], crecv.at[sub, m, kind],
                cs_sem.at[sub, m, kind], cr_sem.at[sub, m, kind], across))
        return copies

    def pack_first(k, x, packed):
        return jnp.where(lane == cols - 1 - k, pltpu.roll(x, cols - 1 - k, 1), packed)

    def pack_last(k, x, packed):
        shift = cols - k if not isinstance(k, int) or k > 0 else 0
        return jnp.where(lane == cols - 1 - k, pltpu.roll(x, shift, 1), packed)

    def pack_inputs(m):
        def one(k, c):
            last, first, ufirst = c
            pk = p[m, k]
            first = pack_first(k, pk, first)
            last = jnp.where(lane == cols - 1 - k, pltpu.roll(pk, lax.rem(cols - k, cols), 1), last)
            ufirst = pack_first(k, u[m, k], ufirst)
            rsend[0, m, 0, pl.ds(k, 1), :] = p[m, k, rows - 1 : rows, :]
            rsend[0, m, 1, pl.ds(k, 1), :] = p[m, k, 0:1, :]
            rsend[0, m, 2, pl.ds(k, 1), :] = v[m, k, 0:1, :]
            return last, first, ufirst

        packs = unrolled(levels, one, (zero, zero, zero), 5)
        for kind in range(3):
            csend[0, m, kind] = packs[kind]

    def pivots():
        def one(i, c):
            k = i + 1
            below, gprev = c
            b = (vert_ratio * vert_ratio) * s[k]
            r = 1.0 / (1.0 + b + below - below * gprev)
            inv[k] = r
            gk = b * r
            g[k] = gk
            return b, gk

        unrolled(levels - 1, one, ((vert_ratio * vert_ratio) * s[0], zero))

    def forward(sub, m):
        last_sub = sub == SUBSTEPS - 1
        before = crecv[0, m, 2] if sub == 0 else ueast[m]
        ueast[m] = before - horiz_ratio * (crecv[sub, m, 1] - csend[sub, m, 0])
        before = rrecv[0, m, 2] if sub == 0 else vnorth[m]
        vnorth[m] = before - horiz_ratio * (rrecv[sub, m, 1] - rsend[sub, m, 0])

        def level(k):
            pk = p[m, k]
            pw = jnp.where(lane == 0, pltpu.roll(crecv[sub, m, 0], k + 1, 1), pltpu.roll(pk, 1, 1))
            ps = jnp.where(row == 0, rrecv[sub, m, 0, pl.ds(k, 1), :], pltpu.roll(pk, 1, 0))
            uk = u[m, k] - horiz_ratio * (pk - pw)
            vk = v[m, k] - horiz_ratio * (pk - ps)
            ue = jnp.where(lane == cols - 1, pltpu.roll(ueast[m], k, 1), pltpu.roll(uk, cols - 1, 1))
            vn = jnp.where(row == rows - 1, vnorth[m, pl.ds(k, 1), :], pltpu.roll(vk, rows - 1, 0))
            part = pk - horiz_ratio * s[k] * ((ue - uk) + (vn - vk))
            if not last_sub:
                u[m, k] = uk
                v[m, k] = vk
            p[m, k] = part
            return uk, vk, part

        def one(i, c):
            k = i + 1
            part_below, value, usum, vsum = c
            uk, vk, part = level(k)
            rhs = w[m, i] - vert_ratio * (part - part_below)
            value = (rhs + (vert_ratio * vert_ratio) * s[i] * value) * inv[k]
            w[m, i] = value
            if last_sub:
                usum = usum + thick[k] * uk
                vsum = vsum + thick[k] * vk
            return part, value, usum, vsum

        uk, vk, part = level(0)
        if last_sub:
            sums = (thick[0] * uk, thick[0] * vk)
            c = unrolled(levels - 1, one, (part, zero) + sums)
            return c[2], c[3]

        def two(i, c):
            return one(i, c + (None, None))[:2]

        unrolled(levels - 1, two, (part, zero))
        return None

    def backward(sub, m):
        last_sub = sub == SUBSTEPS - 1

        def finish(k, pk, c):
            if last_sub:
                return (c[0] + thick[k] * pk,)
            p[m, k] = pk
            rsend[sub + 1, m, 0, pl.ds(k, 1), :] = pk[rows - 1 : rows, :]
            rsend[sub + 1, m, 1, pl.ds(k, 1), :] = pk[0:1, :]
            return pack_last(k, pk, c[0]), pack_first(k, pk, c[1])

        def one(i, c):
            k = levels - 1 - i
            above = c[0]
            here = w[m, k - 1] + g[k] * above
            if not last_sub:
                w[m, k - 1] = here
            pk = p[m, k] - vert_ratio * s[k] * (above - here)
            return (here,) + finish(k, pk, c[1:])

        c = unrolled(levels - 1, one, (zero,) * (2 if last_sub else 3))
        pk = p[m, 0] - vert_ratio * s[0] * c[0]
        c = finish(0, pk, c[1:])
        if last_sub:
            return c[0]
        csend[sub + 1, m, 0] = c[0]
        csend[sub + 1, m, 1] = c[1]
        return None

    sent = []

    def send_halos(sub, m):
        for copy in halo_copies(sub, m):
            copy.start()
            sent.append(copy)

    for m in range(own):
        for name in "puv":
            loads[name, m].wait()
        pack_inputs(m)
        if m == 0:
            pl.semaphore_wait(barrier, tiles - 1 + n_mem - 1)
        send_halos(0, m)
        if m == 0:
            loads["s"].wait()
            pivots()

    for sub in range(SUBSTEPS):
        for m in range(own):
            if sub == 0:
                loads["w", m].wait()
            for copy in halo_copies(sub, m):
                copy.wait_recv()
            sums = forward(sub, m)
            mass = backward(sub, m)
            if sub < SUBSTEPS - 1:
                send_halos(sub + 1, m)
                continue
            for f, total in enumerate((mass,) + sums):
                for q in range(n_mem):
                    integ[m, q, f] = total[q * quarter : (q + 1) * quarter]
            for i in range(1, n_mem):
                other, where = mem_id(i)
                copy = remote(
                    integ.at[m, other], gath.at[mem, m], ms_sem.at[m, other], mr_sem.at[m, mem], where)
                copy.start()
                sent.append(copy)

    fields = [[integ[m, mem, f] for f in range(3)] for m in range(own)]
    for m in range(own):
        for i in range(1, n_mem):
            other, where = mem_id(i)
            remote(integ.at[m, other], gath.at[other, m], ms_sem.at[m, other], mr_sem.at[m, other], where).wait_recv()
            fields.append([gath[other, m, f] for f in range(3)])
    members = len(fields)
    for f in range(3):
        total = fields[0][f]
        for one in fields[1:]:
            total = total + one[f]
        mean = total / members
        second = (fields[0][f] - mean) ** 2
        for one in fields[1:]:
            second = second + (one[f] - mean) ** 2
        everyone[me, f] = mean
        everyone[me, 3 + f] = second / (members - 1)

    for i in range(1, tiles):
        other, where = tile_id(i)
        copy = remote(everyone.at[me], everyone.at[me], as_sem.at[i], ar_sem.at[me], where)
        copy.start()
        sent.append(copy)
    mine = jnp.int32(0)
    for t in range(tiles):
        mine = jnp.where(owner[t] == me, t, mine)
    for i in range(1, tiles):
        other, where = tile_id(i)
        remote(everyone.at[me], everyone.at[other], as_sem.at[i], ar_sem.at[other], where).wait_recv()
    out[0, 0] = everyone[mine]
    for copy in sent:
        copy.wait_send()


def solution(mesh):
    n_mem, n_ty, n_tx = (mesh.shape[a] for a in ("mem", "ty", "tx"))
    tiles = n_ty * n_tx

    def local(pressure, east_wind, north_wind, vertical_wind, sound_squared, thickness, owner_map):
        own, levels, rows, cols = pressure.shape
        quarter = rows // n_mem
        f32 = jnp.float32
        dma = pltpu.SemaphoreType.DMA
        anywhere = pl.BlockSpec(memory_space=pl.ANY)
        scalars = pl.BlockSpec(memory_space=pltpu.SMEM)
        return pl.pallas_call(
            functools.partial(kernel, (n_mem, n_ty, n_tx)),
            name="acoustic",
            out_shape=jax.ShapeDtypeStruct((1, 1, 6, quarter, cols), f32),
            in_specs=[anywhere] * 5 + [scalars] * 2,
            out_specs=pl.BlockSpec(memory_space=pltpu.VMEM),
            scratch_shapes=[
                pltpu.VMEM((own, levels, rows, cols), f32),
                pltpu.VMEM((own, levels, rows, cols), f32),
                pltpu.VMEM((own, levels, rows, cols), f32),
                pltpu.VMEM((own, levels - 1, rows, cols), f32),
                pltpu.VMEM((levels, rows, cols), f32),
                pltpu.VMEM((levels, rows, cols), f32),
                pltpu.VMEM((levels, rows, cols), f32),
                pltpu.VMEM((SUBSTEPS, own, 3, rows, cols), f32),
                pltpu.VMEM((SUBSTEPS, own, 3, rows, cols), f32),
                pltpu.VMEM((SUBSTEPS, own, 3, levels, cols), f32),
                pltpu.VMEM((SUBSTEPS, own, 3, levels, cols), f32),
                pltpu.VMEM((own, rows, cols), f32),
                pltpu.VMEM((own, levels, cols), f32),
                pltpu.VMEM((own, n_mem, 3, quarter, cols), f32),
                pltpu.VMEM((n_mem, own, 3, quarter, cols), f32),
                pltpu.VMEM((tiles, 6, quarter, cols), f32),
                dma((4 * own + 1,)),
                dma((SUBSTEPS, own, 3)),
                dma((SUBSTEPS, own, 3)),
                dma((SUBSTEPS, own, 3)),
                dma((SUBSTEPS, own, 3)),
                dma((own, n_mem)),
                dma((own, n_mem)),
                dma((tiles,)),
                dma((tiles,)),
            ],
            compiler_params=pltpu.CompilerParams(collective_id=0, has_side_effects=True),
        )(pressure, east_wind, north_wind, vertical_wind, sound_squared, thickness, owner_map)

    field = P("mem", None, "ty", "tx")
    return jax.shard_map(
        local,
        mesh=mesh,
        in_specs=(field, field, field, field, P(None, "ty", "tx"), P(), P()),
        out_specs=P("ty", "tx", None, "mem", None),
        check_vma=False,
    )
```

```python
import functools

import jax
import jax.numpy as jnp
from jax import lax
from jax.experimental import pallas as pl
from jax.experimental.pallas import tpu as pltpu
from jax.sharding import PartitionSpec as P

SUBSTEPS = 2
MESH = pl.DeviceIdType.MESH

horiz_ratio = 0.35
vert_ratio = 1.5


def unrolled(count, body, carry, most=7):
    width = max(d for d in range(1, most + 1) if count % d == 0)

    def block(i, c):
        for j in range(width):
            c = body(i * width + j, c)
        return c

    return lax.fori_loop(0, count // width, block, carry)


def kernel(
    sizes,
    p_hbm, u_hbm, v_hbm, w_hbm, s_hbm, thick, owner,
    out,
    p, u, v, w, s, inv, g, lam, sig, alpha, edge_cols, edge_rows,
    csend, crecv, rsend, rrecv, ueast, vnorth,
    integ, gath, everyone,
    load_sem, cs_sem, cr_sem, rs_sem, rr_sem, ms_sem, mr_sem, as_sem, ar_sem,
):
    n_mem, n_ty, n_tx = sizes
    own, levels, rows, cols = p.shape
    quarter = rows // n_mem
    tiles = n_ty * n_tx
    mem, ty, tx = lax.axis_index("mem"), lax.axis_index("ty"), lax.axis_index("tx")
    me = ty * n_tx + tx
    east, west = {"tx": lax.rem(tx + 1, n_tx)}, {"tx": lax.rem(tx + n_tx - 1, n_tx)}
    north, south = {"ty": lax.rem(ty + 1, n_ty)}, {"ty": lax.rem(ty + n_ty - 1, n_ty)}
    lane = lax.broadcasted_iota(jnp.int32, (rows, cols), 1)
    row = lax.broadcasted_iota(jnp.int32, (rows, cols), 0)
    zero = jnp.zeros((rows, cols), jnp.float32)
    lane8 = lax.broadcasted_iota(jnp.int32, (8, cols), 1)
    zero8 = jnp.zeros((8, cols), jnp.float32)

    def load(src, dst, sem):
        copy = pltpu.make_async_copy(src, dst, load_sem.at[sem])
        copy.start()
        return copy

    loads = {"s": load(s_hbm, s, 4 * own)}
    for m in range(own):
        for i, (name, src, dst) in enumerate((("p", p_hbm, p), ("u", u_hbm, u), ("v", v_hbm, v))):
            loads[name, m] = load(src.at[m], dst.at[m], 4 * m + i)
    for m in range(own):
        loads["w", m] = load(w_hbm.at[m], w.at[m], 4 * m + 3)

    barrier = pltpu.get_barrier_semaphore()

    def tile_id(i):
        other = lax.rem(me + i, tiles)
        return other, {"ty": lax.div(other, n_tx), "tx": lax.rem(other, n_tx)}

    def mem_id(i):
        other = lax.rem(mem + i, n_mem)
        return other, {"mem": other}

    for i in range(1, tiles):
        pl.semaphore_signal(barrier, inc=1, device_id=tile_id(i)[1], device_id_type=MESH)
    for i in range(1, n_mem):
        pl.semaphore_signal(barrier, inc=1, device_id=mem_id(i)[1], device_id_type=MESH)

    def remote(src, dst, ssem, rsem, where):
        return pltpu.make_async_remote_copy(
            src_ref=src, dst_ref=dst, send_sem=ssem, recv_sem=rsem, device_id=where, device_id_type=MESH
        )

    def halo_copies(sub, m):
        kinds = ((0, east, north), (1, west, south), (2, west, south))
        copies = []
        for kind, across, along in kinds if sub == 0 else kinds[:2]:
            copies.append(remote(
                rsend.at[sub, m, kind], rrecv.at[sub, m, kind],
                rs_sem.at[sub, m, kind], rr_sem.at[sub, m, kind], along))
            copies.append(remote(
                csend.at[sub, m, kind], crecv.at[sub, m, kind],
                cs_sem.at[sub, m, kind], cr_sem.at[sub, m, kind], across))
        return copies

    def pack_first(k, x, packed):
        return jnp.where(lane == cols - 1 - k, pltpu.roll(x, cols - 1 - k, 1), packed)

    def pack_last(k, x, packed):
        shift = cols - k if not isinstance(k, int) or k > 0 else 0
        return jnp.where(lane == cols - 1 - k, pltpu.roll(x, shift, 1), packed)

    def pack_inputs(m):
        def one(k, c):
            last, first, ufirst = c
            pk = p[m, k]
            first = pack_first(k, pk, first)
            last = jnp.where(lane == cols - 1 - k, pltpu.roll(pk, lax.rem(cols - k, cols), 1), last)
            ufirst = pack_first(k, u[m, k], ufirst)
            rsend[0, m, 0, pl.ds(k, 1), :] = p[m, k, rows - 1 : rows, :]
            rsend[0, m, 1, pl.ds(k, 1), :] = p[m, k, 0:1, :]
            rsend[0, m, 2, pl.ds(k, 1), :] = v[m, k, 0:1, :]
            return last, first, ufirst

        packs = unrolled(levels, one, (zero, zero, zero), 5)
        for kind in range(3):
            csend[0, m, kind] = packs[kind]

    def pivots():
        def one(i, c):
            k = i + 1
            below, gprev, mass_below, value = c
            sk = s[k]
            b = (vert_ratio * vert_ratio) * sk
            mass = thick[k] * sk
            r = 1.0 / (1.0 + b + below - below * gprev)
            gk = b * r
            value = (vert_ratio * (mass - mass_below) + below * value) * r
            inv[k] = r
            g[k] = gk
            lam[k] = value
            return b, gk, mass, value

        unrolled(levels - 1, one, ((vert_ratio * vert_ratio) * s[0], zero, thick[0] * s[0], zero))

        def weights(k, here, above, first, last, mass):
            mu = thick[k] - vert_ratio * (here - above)
            sk = (horiz_ratio * horiz_ratio) * mu * s[k]
            sig[k] = sk
            alpha[k] = mu - 4.0 * sk
            edge_rows[0, pl.ds(k, 1), :] = sk[0:1, :]
            edge_rows[1, pl.ds(k, 1), :] = sk[rows - 1 : rows, :]
            edge_rows[2, pl.ds(k, 1), :] = jnp.zeros((1, cols), jnp.float32) + thick[k]
            mass = jnp.where(lane8 == cols - 1 - k, thick[k], mass)
            return pack_first(k, sk, first), pack_last(k, sk, last), mass

        def two(i, c):
            k = levels - 1 - i
            here = lam[k] + g[k] * c[0]
            lam[k] = here
            return (here,) + weights(k, here, *c)

        c = unrolled(levels - 1, two, (zero, zero, zero, zero8))
        first, last, mass = weights(0, zero, *c)
        edge_cols[0] = first
        edge_cols[1] = last
        edge_cols[2] = jnp.concatenate([mass] * (rows // 8), axis=0)

    def forward(m):
        ueast[m] = crecv[0, m, 2] - horiz_ratio * (crecv[0, m, 1] - csend[0, m, 0])
        vnorth[m] = rrecv[0, m, 2] - horiz_ratio * (rrecv[0, m, 1] - rsend[0, m, 0])

        def level(k, usum, vsum, dsum):
            pk = p[m, k]
            pw = jnp.where(lane == 0, pltpu.roll(crecv[0, m, 0], k + 1, 1), pltpu.roll(pk, 1, 1))
            ps = jnp.where(row == 0, rrecv[0, m, 0, pl.ds(k, 1), :], pltpu.roll(pk, 1, 0))
            uk = u[m, k] - horiz_ratio * (pk - pw)
            vk = v[m, k] - horiz_ratio * (pk - ps)
            ue = jnp.where(lane == cols - 1, pltpu.roll(ueast[m], k, 1), pltpu.roll(uk, cols - 1, 1))
            vn = jnp.where(row == rows - 1, vnorth[m, pl.ds(k, 1), :], pltpu.roll(vk, rows - 1, 0))
            div = (ue - uk) + (vn - vk)
            part = pk - horiz_ratio * s[k] * div
            p[m, k] = part
            return part, usum + thick[k] * uk, vsum + thick[k] * vk, dsum + sig[k] * div

        def one(i, c):
            k = i + 1
            part_below, value = c[:2]
            part, *sums = level(k, *c[2:])
            rhs = w[m, i] - vert_ratio * (part - part_below)
            value = (rhs + (vert_ratio * vert_ratio) * s[i] * value) * inv[k]
            w[m, i] = value
            return (part, value, *sums)

        part, *sums = level(0, zero, zero, zero)
        return unrolled(levels - 1, one, (part, zero, *sums))[2:]

    def backward(m):
        def finish(k, pk, c):
            last, first, mass, total = c
            rsend[1, m, 0, pl.ds(k, 1), :] = pk[rows - 1 : rows, :]
            rsend[1, m, 1, pl.ds(k, 1), :] = pk[0:1, :]
            around = (pltpu.roll(pk, 1, 1) + pltpu.roll(pk, cols - 1, 1)) + (
                pltpu.roll(pk, 1, 0) + pltpu.roll(pk, rows - 1, 0))
            total = total + (alpha[k] * pk + sig[k] * around)
            return pack_last(k, pk, last), pack_first(k, pk, first), mass + thick[k] * pk, total

        def one(i, c):
            k = levels - 1 - i
            above = c[0]
            here = w[m, k - 1] + g[k] * above
            pk = p[m, k] - vert_ratio * s[k] * (above - here)
            last, first, mass, total = finish(k, pk, c[1:])
            return here, last, first, mass, total + lam[k] * here

        c = unrolled(levels - 1, one, (zero,) * 5)
        pk = p[m, 0] - vert_ratio * s[0] * c[0]
        last, first, mass, total = finish(0, pk, c[1:])
        csend[1, m, 0] = last
        csend[1, m, 1] = first
        return mass, total

    def integrals(m, usum, vsum, dsum, mass, total):
        across = lambda x: jnp.sum(x, axis=1, keepdims=True)
        along = lambda x: jnp.sum(x, axis=0, keepdims=True)
        pw, ps = crecv[1, m, 0], rrecv[1, m, 0]
        total = total - dsum / horiz_ratio
        total = total + jnp.where(lane == 0, across(edge_cols[0] * (pw - csend[1, m, 0])), 0.0)
        total = total + jnp.where(
            lane == cols - 1, across(edge_cols[1] * (crecv[1, m, 1] - csend[1, m, 1])), 0.0)
        total = total + jnp.where(row == 0, along(edge_rows[0] * (ps - rsend[1, m, 0])), 0.0)
        total = total + jnp.where(
            row == rows - 1, along(edge_rows[1] * (rrecv[1, m, 1] - rsend[1, m, 1])), 0.0)
        mass_west = jnp.where(lane == 0, across(edge_cols[2] * pw), pltpu.roll(mass, 1, 1))
        mass_south = jnp.where(row == 0, along(edge_rows[2] * ps), pltpu.roll(mass, 1, 0))
        return (
            total,
            usum - horiz_ratio * (mass - mass_west),
            vsum - horiz_ratio * (mass - mass_south),
        )

    sent = []

    def send_halos(sub, m):
        for copy in halo_copies(sub, m):
            copy.start()
            sent.append(copy)

    loads["s"].wait()
    pivots()
    for m in range(own):
        for name in "puv":
            loads[name, m].wait()
        pack_inputs(m)
        if m == 0:
            pl.semaphore_wait(barrier, tiles - 1 + n_mem - 1)
        send_halos(0, m)

    sums = []
    for m in range(own):
        loads["w", m].wait()
        for copy in halo_copies(0, m):
            copy.wait_recv()
        sums.append((*forward(m), *backward(m)))
        send_halos(1, m)
    for m in range(own):
        for copy in halo_copies(1, m):
            copy.wait_recv()
        for f, total in enumerate(integrals(m, *sums[m])):
            for q in range(n_mem):
                integ[m, q, f] = total[q * quarter : (q + 1) * quarter]
        for i in range(1, n_mem):
            other, where = mem_id(i)
            copy = remote(
                integ.at[m, other], gath.at[mem, m], ms_sem.at[m, other], mr_sem.at[m, mem], where)
            copy.start()
            sent.append(copy)

    fields = [[integ[m, mem, f] for f in range(3)] for m in range(own)]
    for m in range(own):
        for i in range(1, n_mem):
            other, where = mem_id(i)
            remote(integ.at[m, other], gath.at[other, m], ms_sem.at[m, other], mr_sem.at[m, other], where).wait_recv()
            fields.append([gath[other, m, f] for f in range(3)])
    members = len(fields)
    for f in range(3):
        total = fields[0][f]
        for one in fields[1:]:
            total = total + one[f]
        mean = total / members
        second = (fields[0][f] - mean) ** 2
        for one in fields[1:]:
            second = second + (one[f] - mean) ** 2
        everyone[me, f] = mean
        everyone[me, 3 + f] = second / (members - 1)

    for i in range(1, tiles):
        other, where = tile_id(i)
        copy = remote(everyone.at[me], everyone.at[me], as_sem.at[i], ar_sem.at[me], where)
        copy.start()
        sent.append(copy)
    mine = jnp.int32(0)
    for t in range(tiles):
        mine = jnp.where(owner[t] == me, t, mine)
    for i in range(1, tiles):
        other, where = tile_id(i)
        remote(everyone.at[me], everyone.at[other], as_sem.at[i], ar_sem.at[other], where).wait_recv()
    out[0, 0] = everyone[mine]
    for copy in sent:
        copy.wait_send()


def solution(mesh):
    n_mem, n_ty, n_tx = (mesh.shape[a] for a in ("mem", "ty", "tx"))
    tiles = n_ty * n_tx

    def local(pressure, east_wind, north_wind, vertical_wind, sound_squared, thickness, owner_map):
        own, levels, rows, cols = pressure.shape
        quarter = rows // n_mem
        f32 = jnp.float32
        dma = pltpu.SemaphoreType.DMA
        anywhere = pl.BlockSpec(memory_space=pl.ANY)
        scalars = pl.BlockSpec(memory_space=pltpu.SMEM)
        return pl.pallas_call(
            functools.partial(kernel, (n_mem, n_ty, n_tx)),
            name="acoustic",
            out_shape=jax.ShapeDtypeStruct((1, 1, 6, quarter, cols), f32),
            in_specs=[anywhere] * 5 + [scalars] * 2,
            out_specs=pl.BlockSpec(memory_space=pltpu.VMEM),
            scratch_shapes=[
                pltpu.VMEM((own, levels, rows, cols), f32),
                pltpu.VMEM((own, levels, rows, cols), f32),
                pltpu.VMEM((own, levels, rows, cols), f32),
                pltpu.VMEM((own, levels - 1, rows, cols), f32),
                *[pltpu.VMEM((levels, rows, cols), f32)] * 6,
                pltpu.VMEM((3, rows, cols), f32),
                pltpu.VMEM((3, levels, cols), f32),
                pltpu.VMEM((SUBSTEPS, own, 3, rows, cols), f32),
                pltpu.VMEM((SUBSTEPS, own, 3, rows, cols), f32),
                pltpu.VMEM((SUBSTEPS, own, 3, levels, cols), f32),
                pltpu.VMEM((SUBSTEPS, own, 3, levels, cols), f32),
                pltpu.VMEM((own, rows, cols), f32),
                pltpu.VMEM((own, levels, cols), f32),
                pltpu.VMEM((own, n_mem, 3, quarter, cols), f32),
                pltpu.VMEM((n_mem, own, 3, quarter, cols), f32),
                pltpu.VMEM((tiles, 6, quarter, cols), f32),
                dma((4 * own + 1,)),
                dma((SUBSTEPS, own, 3)),
                dma((SUBSTEPS, own, 3)),
                dma((SUBSTEPS, own, 3)),
                dma((SUBSTEPS, own, 3)),
                dma((own, n_mem)),
                dma((own, n_mem)),
                dma((tiles,)),
                dma((tiles,)),
            ],
            compiler_params=pltpu.CompilerParams(collective_id=0, has_side_effects=True),
        )(pressure, east_wind, north_wind, vertical_wind, sound_squared, thickness, owner_map)

    field = P("mem", None, "ty", "tx")
    return jax.shard_map(
        local,
        mesh=mesh,
        in_specs=(field, field, field, field, P(None, "ty", "tx"), P(), P()),
        out_specs=P("ty", "tx", None, "mem", None),
        check_vma=False,
    )
```

```python
import functools

import jax
import jax.numpy as jnp
from jax import lax
from jax.experimental import pallas as pl
from jax.experimental.pallas import tpu as pltpu
from jax.sharding import PartitionSpec as P

SUBSTEPS = 2
MESH = pl.DeviceIdType.MESH

horiz_ratio = 0.35
vert_ratio = 1.5


def unrolled(count, body, carry, most=7):
    width = max(d for d in range(1, most + 1) if count % d == 0)

    def block(i, c):
        for j in range(width):
            c = body(i * width + j, c)
        return c

    return lax.fori_loop(0, count // width, block, carry)


def kernel(
    sizes,
    p_hbm, u_hbm, v_hbm, w_hbm, s_hbm, thick, owner,
    out,
    p, u, v, w, s, inv, g, lam, sig, alpha, edge_cols, edge_rows,
    csend, crecv, rsend, rrecv, ueast, vnorth,
    integ, gath, everyone,
    load_sem, cs_sem, cr_sem, rs_sem, rr_sem, ms_sem, mr_sem, as_sem, ar_sem,
):
    n_mem, n_ty, n_tx = sizes
    own, levels, rows, cols = p.shape
    quarter = rows // n_mem
    tiles = n_ty * n_tx
    mem, ty, tx = lax.axis_index("mem"), lax.axis_index("ty"), lax.axis_index("tx")
    me = ty * n_tx + tx
    east, west = {"tx": lax.rem(tx + 1, n_tx)}, {"tx": lax.rem(tx + n_tx - 1, n_tx)}
    north, south = {"ty": lax.rem(ty + 1, n_ty)}, {"ty": lax.rem(ty + n_ty - 1, n_ty)}
    lane = lax.broadcasted_iota(jnp.int32, (rows, cols), 1)
    row = lax.broadcasted_iota(jnp.int32, (rows, cols), 0)
    zero = jnp.zeros((rows, cols), jnp.float32)
    lane8 = lax.broadcasted_iota(jnp.int32, (8, cols), 1)
    zero8 = jnp.zeros((8, cols), jnp.float32)

    def load(src, dst, sem):
        copy = pltpu.make_async_copy(src, dst, load_sem.at[sem])
        copy.start()
        return copy

    loads = {"s": load(s_hbm, s, 4 * own)}
    for m in range(own):
        for i, (name, src, dst) in enumerate((("p", p_hbm, p), ("u", u_hbm, u), ("v", v_hbm, v))):
            loads[name, m] = load(src.at[m], dst.at[m], 4 * m + i)
    for m in range(own):
        loads["w", m] = load(w_hbm.at[m], w.at[m], 4 * m + 3)

    barrier = pltpu.get_barrier_semaphore()

    far = lambda d: -(min(d[0], n_ty - d[0]) + min(d[1], n_tx - d[1]))
    offsets = sorted([(a, b) for a in range(n_ty) for b in range(n_tx)], key=far)

    def tile_id(i):
        a, b = offsets[i - 1]
        other_ty, other_tx = lax.rem(ty + a, n_ty), lax.rem(tx + b, n_tx)
        return other_ty * n_tx + other_tx, {"ty": other_ty, "tx": other_tx}

    def mem_id(i):
        other = lax.rem(mem + i, n_mem)
        return other, {"mem": other}

    for i in range(1, tiles):
        pl.semaphore_signal(barrier, inc=1, device_id=tile_id(i)[1], device_id_type=MESH)
    for i in range(1, n_mem):
        pl.semaphore_signal(barrier, inc=1, device_id=mem_id(i)[1], device_id_type=MESH)

    def remote(src, dst, ssem, rsem, where):
        return pltpu.make_async_remote_copy(
            src_ref=src, dst_ref=dst, send_sem=ssem, recv_sem=rsem, device_id=where, device_id_type=MESH
        )

    def halo_copies(sub, m):
        kinds = ((0, east, north), (1, west, south))
        copies = []
        for kind, across, along in kinds:
            copies.append(remote(
                rsend.at[sub, m, kind], rrecv.at[sub, m, kind],
                rs_sem.at[sub, m, kind], rr_sem.at[sub, m, kind], along))
            copies.append(remote(
                csend.at[sub, m, kind], crecv.at[sub, m, kind],
                cs_sem.at[sub, m, kind], cr_sem.at[sub, m, kind], across))
        return copies

    def pack_first(k, x, packed):
        return jnp.where(lane == cols - 1 - k, pltpu.roll(x, cols - 1 - k, 1), packed)

    def pack_last(k, x, packed):
        shift = cols - k if not isinstance(k, int) or k > 0 else 0
        return jnp.where(lane == cols - 1 - k, pltpu.roll(x, shift, 1), packed)

    def pack_inputs(m):
        def one(k, c):
            last, first = c
            pk = p[m, k]
            first = pack_first(k, u[m, k] - horiz_ratio * pk, first)
            last = jnp.where(lane == cols - 1 - k, pltpu.roll(pk, lax.rem(cols - k, cols), 1), last)
            rsend[0, m, 0, pl.ds(k, 1), :] = p[m, k, rows - 1 : rows, :]
            rsend[0, m, 1, pl.ds(k, 1), :] = v[m, k, 0:1, :] - horiz_ratio * p[m, k, 0:1, :]
            return last, first

        packs = unrolled(levels, one, (zero, zero), 5)
        for kind in range(2):
            csend[0, m, kind] = packs[kind]

    def pivots():
        def one(i, c):
            k = i + 1
            below, gprev, mass_below, value = c
            sk = s[k]
            b = (vert_ratio * vert_ratio) * sk
            mass = thick[k] * sk
            r = 1.0 / (1.0 + b + below - below * gprev)
            gk = b * r
            value = (vert_ratio * (mass - mass_below) + below * value) * r
            inv[k] = r
            g[k] = gk
            lam[k] = value
            return b, gk, mass, value

        unrolled(levels - 1, one, ((vert_ratio * vert_ratio) * s[0], zero, thick[0] * s[0], zero))

        def weights(k, here, above, first, last, mass):
            mu = thick[k] - vert_ratio * (here - above)
            sk = (horiz_ratio * horiz_ratio) * mu * s[k]
            sig[k] = sk
            alpha[k] = mu - 4.0 * sk
            edge_rows[0, pl.ds(k, 1), :] = sk[0:1, :]
            edge_rows[1, pl.ds(k, 1), :] = sk[rows - 1 : rows, :]
            edge_rows[2, pl.ds(k, 1), :] = jnp.zeros((1, cols), jnp.float32) + thick[k]
            mass = jnp.where(lane8 == cols - 1 - k, thick[k], mass)
            return pack_first(k, sk, first), pack_last(k, sk, last), mass

        def two(i, c):
            k = levels - 1 - i
            here = lam[k] + g[k] * c[0]
            lam[k] = here
            return (here,) + weights(k, here, *c)

        c = unrolled(levels - 1, two, (zero, zero, zero, zero8))
        first, last, mass = weights(0, zero, *c)
        edge_cols[0] = first
        edge_cols[1] = last
        edge_cols[2] = jnp.concatenate([mass] * (rows // 8), axis=0)

    def forward(m):
        ueast[m] = crecv[0, m, 1] + horiz_ratio * csend[0, m, 0]
        vnorth[m] = rrecv[0, m, 1] + horiz_ratio * rsend[0, m, 0]

        def level(k, usum, vsum, dsum):
            pk = p[m, k]
            pw = jnp.where(lane == 0, pltpu.roll(crecv[0, m, 0], k + 1, 1), pltpu.roll(pk, 1, 1))
            ps = jnp.where(row == 0, rrecv[0, m, 0, pl.ds(k, 1), :], pltpu.roll(pk, 1, 0))
            uk = u[m, k] - horiz_ratio * (pk - pw)
            vk = v[m, k] - horiz_ratio * (pk - ps)
            ue = jnp.where(lane == cols - 1, pltpu.roll(ueast[m], k, 1), pltpu.roll(uk, cols - 1, 1))
            vn = jnp.where(row == rows - 1, vnorth[m, pl.ds(k, 1), :], pltpu.roll(vk, rows - 1, 0))
            div = (ue - uk) + (vn - vk)
            part = pk - horiz_ratio * s[k] * div
            p[m, k] = part
            return part, usum + thick[k] * uk, vsum + thick[k] * vk, dsum + sig[k] * div

        def one(i, c):
            k = i + 1
            part_below, value = c[:2]
            part, *sums = level(k, *c[2:])
            rhs = w[m, i] - vert_ratio * (part - part_below)
            value = (rhs + (vert_ratio * vert_ratio) * s[i] * value) * inv[k]
            w[m, i] = value
            return (part, value, *sums)

        part, *sums = level(0, zero, zero, zero)
        return unrolled(levels - 1, one, (part, zero, *sums))[2:]

    def backward(m):
        def finish(k, pk, last, first):
            p[m, k] = pk
            rsend[1, m, 0, pl.ds(k, 1), :] = pk[rows - 1 : rows, :]
            rsend[1, m, 1, pl.ds(k, 1), :] = pk[0:1, :]
            return pack_last(k, pk, last), pack_first(k, pk, first)

        def one(i, c):
            k = levels - 1 - i
            above = c[0]
            here = w[m, k - 1] + g[k] * above
            w[m, k - 1] = here
            pk = p[m, k] - vert_ratio * s[k] * (above - here)
            return (here,) + finish(k, pk, c[1], c[2])

        c = unrolled(levels - 1, one, (zero,) * 3)
        last, first = finish(0, p[m, 0] - vert_ratio * s[0] * c[0], c[1], c[2])
        csend[1, m, 0] = last
        csend[1, m, 1] = first

    def weigh(m):
        def level(k, mass, total):
            pk = p[m, k]
            around = (pltpu.roll(pk, 1, 1) + pltpu.roll(pk, cols - 1, 1)) + (
                pltpu.roll(pk, 1, 0) + pltpu.roll(pk, rows - 1, 0))
            return mass + thick[k] * pk, total + (alpha[k] * pk + sig[k] * around)

        def one(i, c):
            mass, total = level(i + 1, *c)
            return mass, total + lam[i + 1] * w[m, i]

        return unrolled(levels - 1, one, level(0, zero, zero))

    def integrals(m, usum, vsum, dsum, mass, total):
        across = lambda x: jnp.sum(x, axis=1, keepdims=True)
        along = lambda x: jnp.sum(x, axis=0, keepdims=True)
        pw, ps = crecv[1, m, 0], rrecv[1, m, 0]
        total = total - dsum / horiz_ratio
        total = total + jnp.where(lane == 0, across(edge_cols[0] * (pw - csend[1, m, 0])), 0.0)
        total = total + jnp.where(
            lane == cols - 1, across(edge_cols[1] * (crecv[1, m, 1] - csend[1, m, 1])), 0.0)
        total = total + jnp.where(row == 0, along(edge_rows[0] * (ps - rsend[1, m, 0])), 0.0)
        total = total + jnp.where(
            row == rows - 1, along(edge_rows[1] * (rrecv[1, m, 1] - rsend[1, m, 1])), 0.0)
        mass_west = jnp.where(lane == 0, across(edge_cols[2] * pw), pltpu.roll(mass, 1, 1))
        mass_south = jnp.where(row == 0, along(edge_rows[2] * ps), pltpu.roll(mass, 1, 0))
        return (
            total,
            usum - horiz_ratio * (mass - mass_west),
            vsum - horiz_ratio * (mass - mass_south),
        )

    sent = []

    def send_halos(sub, m):
        for copy in halo_copies(sub, m):
            copy.start()
            sent.append(copy)

    loads["s"].wait()
    pivots()
    for m in range(own):
        for name in "puv":
            loads[name, m].wait()
        pack_inputs(m)
        if m == 0:
            pl.semaphore_wait(barrier, tiles - 1 + n_mem - 1)
        send_halos(0, m)

    sums = []
    for m in range(own):
        loads["w", m].wait()
        for copy in halo_copies(0, m):
            copy.wait_recv()
        sums.append(forward(m))
        backward(m)
        send_halos(1, m)
    sums = [(*sums[m], *weigh(m)) for m in range(own)]
    for m in range(own):
        for copy in halo_copies(1, m):
            copy.wait_recv()
        for f, total in enumerate(integrals(m, *sums[m])):
            for q in range(n_mem):
                integ[m, q, f] = total[q * quarter : (q + 1) * quarter]
        for i in range(1, n_mem):
            other, where = mem_id(i)
            copy = remote(
                integ.at[m, other], gath.at[mem, m], ms_sem.at[m, other], mr_sem.at[m, mem], where)
            copy.start()
            sent.append(copy)

    fields = [[integ[m, mem, f] for f in range(3)] for m in range(own)]
    for m in range(own):
        for i in range(1, n_mem):
            other, where = mem_id(i)
            remote(integ.at[m, other], gath.at[other, m], ms_sem.at[m, other], mr_sem.at[m, other], where).wait_recv()
            fields.append([gath[other, m, f] for f in range(3)])
    members = len(fields)
    for f in range(3):
        total = fields[0][f]
        for one in fields[1:]:
            total = total + one[f]
        mean = total / members
        second = (fields[0][f] - mean) ** 2
        for one in fields[1:]:
            second = second + (one[f] - mean) ** 2
        everyone[me, f] = mean
        everyone[me, 3 + f] = second / (members - 1)

    for i in range(1, tiles):
        other, where = tile_id(i)
        copy = remote(everyone.at[me], everyone.at[me], as_sem.at[i], ar_sem.at[me], where)
        copy.start()
        sent.append(copy)
    mine = jnp.int32(0)
    for t in range(tiles):
        mine = jnp.where(owner[t] == me, t, mine)
    for i in range(1, tiles):
        other, where = tile_id(i)
        remote(everyone.at[me], everyone.at[other], as_sem.at[i], ar_sem.at[other], where).wait_recv()
    out[0, 0] = everyone[mine]
    for copy in sent:
        copy.wait_send()


def solution(mesh):
    n_mem, n_ty, n_tx = (mesh.shape[a] for a in ("mem", "ty", "tx"))
    tiles = n_ty * n_tx

    def local(pressure, east_wind, north_wind, vertical_wind, sound_squared, thickness, owner_map):
        own, levels, rows, cols = pressure.shape
        quarter = rows // n_mem
        f32 = jnp.float32
        dma = pltpu.SemaphoreType.DMA
        anywhere = pl.BlockSpec(memory_space=pl.ANY)
        scalars = pl.BlockSpec(memory_space=pltpu.SMEM)
        return pl.pallas_call(
            functools.partial(kernel, (n_mem, n_ty, n_tx)),
            name="acoustic",
            out_shape=jax.ShapeDtypeStruct((1, 1, 6, quarter, cols), f32),
            in_specs=[anywhere] * 5 + [scalars] * 2,
            out_specs=pl.BlockSpec(memory_space=pltpu.VMEM),
            scratch_shapes=[
                pltpu.VMEM((own, levels, rows, cols), f32),
                pltpu.VMEM((own, levels, rows, cols), f32),
                pltpu.VMEM((own, levels, rows, cols), f32),
                pltpu.VMEM((own, levels - 1, rows, cols), f32),
                *[pltpu.VMEM((levels, rows, cols), f32)] * 6,
                pltpu.VMEM((3, rows, cols), f32),
                pltpu.VMEM((3, levels, cols), f32),
                pltpu.VMEM((SUBSTEPS, own, 2, rows, cols), f32),
                pltpu.VMEM((SUBSTEPS, own, 2, rows, cols), f32),
                pltpu.VMEM((SUBSTEPS, own, 2, levels, cols), f32),
                pltpu.VMEM((SUBSTEPS, own, 2, levels, cols), f32),
                pltpu.VMEM((own, rows, cols), f32),
                pltpu.VMEM((own, levels, cols), f32),
                pltpu.VMEM((own, n_mem, 3, quarter, cols), f32),
                pltpu.VMEM((n_mem, own, 3, quarter, cols), f32),
                pltpu.VMEM((tiles, 6, quarter, cols), f32),
                dma((4 * own + 1,)),
                dma((SUBSTEPS, own, 2)),
                dma((SUBSTEPS, own, 2)),
                dma((SUBSTEPS, own, 2)),
                dma((SUBSTEPS, own, 2)),
                dma((own, n_mem)),
                dma((own, n_mem)),
                dma((tiles,)),
                dma((tiles,)),
            ],
            compiler_params=pltpu.CompilerParams(collective_id=0, has_side_effects=True),
        )(pressure, east_wind, north_wind, vertical_wind, sound_squared, thickness, owner_map)

    field = P("mem", None, "ty", "tx")
    return jax.shard_map(
        local,
        mesh=mesh,
        in_specs=(field, field, field, field, P(None, "ty", "tx"), P(), P()),
        out_specs=P("ty", "tx", None, "mem", None),
        check_vma=False,
    )
```

```python
import functools

import jax
import jax.numpy as jnp
from jax import lax
from jax.experimental import pallas as pl
from jax.experimental.pallas import tpu as pltpu
from jax.sharding import PartitionSpec as P

SUBSTEPS = 2
MESH = pl.DeviceIdType.MESH

horiz_ratio = 0.35
vert_ratio = 1.5


def unrolled(count, body, carry, most=7):
    width = max(d for d in range(1, most + 1) if count % d == 0)

    def block(i, c):
        for j in range(width):
            c = body(i * width + j, c)
        return c

    return lax.fori_loop(0, count // width, block, carry)


def kernel(
    sizes,
    p_hbm, u_hbm, v_hbm, w_hbm, s_hbm, thick, owner,
    out,
    p, u, v, w, s, inv, g, lam, sig, alpha, edge_cols, edge_rows,
    csend, crecv, rsend, rrecv, ueast, vnorth,
    integ, gath, everyone,
    load_sem, cs_sem, cr_sem, rs_sem, rr_sem, ms_sem, mr_sem, as_sem, ar_sem,
):
    n_mem, n_ty, n_tx = sizes
    own, levels, rows, cols = p.shape
    quarter = rows // n_mem
    tiles = n_ty * n_tx
    mem, ty, tx = lax.axis_index("mem"), lax.axis_index("ty"), lax.axis_index("tx")
    me = ty * n_tx + tx
    east, west = {"tx": lax.rem(tx + 1, n_tx)}, {"tx": lax.rem(tx + n_tx - 1, n_tx)}
    north, south = {"ty": lax.rem(ty + 1, n_ty)}, {"ty": lax.rem(ty + n_ty - 1, n_ty)}
    lane = lax.broadcasted_iota(jnp.int32, (rows, cols), 1)
    row = lax.broadcasted_iota(jnp.int32, (rows, cols), 0)
    zero = jnp.zeros((rows, cols), jnp.float32)
    lane8 = lax.broadcasted_iota(jnp.int32, (8, cols), 1)
    zero8 = jnp.zeros((8, cols), jnp.float32)

    def load(src, dst, sem):
        copy = pltpu.make_async_copy(src, dst, load_sem.at[sem])
        copy.start()
        return copy

    loads = {"s": load(s_hbm, s, 4 * own)}
    for m in range(own):
        for i, (name, src, dst) in enumerate((("p", p_hbm, p), ("u", u_hbm, u), ("v", v_hbm, v))):
            loads[name, m] = load(src.at[m], dst.at[m], 4 * m + i)
    for m in range(own):
        loads["w", m] = load(w_hbm.at[m], w.at[m], 4 * m + 3)

    barrier = pltpu.get_barrier_semaphore()

    far = lambda d: -(min(d[0], n_ty - d[0]) + min(d[1], n_tx - d[1]))
    offsets = sorted([(a, b) for a in range(n_ty) for b in range(n_tx)], key=far)

    def tile_id(i):
        a, b = offsets[i - 1]
        other_ty, other_tx = lax.rem(ty + a, n_ty), lax.rem(tx + b, n_tx)
        return other_ty * n_tx + other_tx, {"ty": other_ty, "tx": other_tx}

    def mem_id(i):
        other = lax.rem(mem + i, n_mem)
        return other, {"mem": other}

    for i in range(1, tiles):
        pl.semaphore_signal(barrier, inc=1, device_id=tile_id(i)[1], device_id_type=MESH)
    for i in range(1, n_mem):
        pl.semaphore_signal(barrier, inc=1, device_id=mem_id(i)[1], device_id_type=MESH)

    def remote(src, dst, ssem, rsem, where):
        return pltpu.make_async_remote_copy(
            src_ref=src, dst_ref=dst, send_sem=ssem, recv_sem=rsem, device_id=where, device_id_type=MESH
        )

    def halo_copies(sub, m):
        kinds = ((0, east, north), (1, west, south))
        copies = []
        for kind, across, along in kinds:
            copies.append(remote(
                rsend.at[sub, m, kind], rrecv.at[sub, m, kind],
                rs_sem.at[sub, m, kind], rr_sem.at[sub, m, kind], along))
            copies.append(remote(
                csend.at[sub, m, kind], crecv.at[sub, m, kind],
                cs_sem.at[sub, m, kind], cr_sem.at[sub, m, kind], across))
        return copies

    def pack_first(k, x, packed):
        return jnp.where(lane == cols - 1 - k, pltpu.roll(x, cols - 1 - k, 1), packed)

    def pack_last(k, x, packed):
        shift = cols - k if not isinstance(k, int) or k > 0 else 0
        return jnp.where(lane == cols - 1 - k, pltpu.roll(x, shift, 1), packed)

    def pack_inputs(m):
        def one(k, c):
            last, first, usum, vsum, mass = c
            pk = p[m, k]
            first = pack_first(k, u[m, k] - horiz_ratio * pk, first)
            last = jnp.where(lane == cols - 1 - k, pltpu.roll(pk, lax.rem(cols - k, cols), 1), last)
            rsend[0, m, 0, pl.ds(k, 1), :] = p[m, k, rows - 1 : rows, :]
            rsend[0, m, 1, pl.ds(k, 1), :] = v[m, k, 0:1, :] - horiz_ratio * p[m, k, 0:1, :]
            uk, vk, pk = thick[k] * u[m, k], thick[k] * v[m, k], thick[k] * pk
            return last, first, usum + uk, vsum + vk, mass + pk

        packs = unrolled(levels, one, (zero,) * 5, 5)
        for kind in range(2):
            csend[0, m, kind] = packs[kind]
        return packs[2:]

    def pivots():
        def one(i, c):
            k = i + 1
            below, gprev, mass_below, value = c
            sk = s[k]
            b = (vert_ratio * vert_ratio) * sk
            mass = thick[k] * sk
            r = 1.0 / (1.0 + b + below - below * gprev)
            gk = b * r
            value = (vert_ratio * (mass - mass_below) + below * value) * r
            inv[k] = r
            g[k] = gk
            lam[k] = value
            return b, gk, mass, value

        unrolled(levels - 1, one, ((vert_ratio * vert_ratio) * s[0], zero, thick[0] * s[0], zero))

        def weights(k, here, above, first, last, mass):
            mu = thick[k] - vert_ratio * (here - above)
            sk = (horiz_ratio * horiz_ratio) * mu * s[k]
            sig[k] = sk
            alpha[k] = mu - 4.0 * sk
            edge_rows[0, pl.ds(k, 1), :] = sk[0:1, :]
            edge_rows[1, pl.ds(k, 1), :] = sk[rows - 1 : rows, :]
            edge_rows[2, pl.ds(k, 1), :] = jnp.zeros((1, cols), jnp.float32) + thick[k]
            mass = jnp.where(lane8 == cols - 1 - k, thick[k], mass)
            return pack_first(k, sk, first), pack_last(k, sk, last), mass

        def two(i, c):
            k = levels - 1 - i
            here = lam[k] + g[k] * c[0]
            lam[k] = here
            return (here,) + weights(k, here, *c)

        c = unrolled(levels - 1, two, (zero, zero, zero, zero8))
        first, last, mass = weights(0, zero, *c)
        edge_cols[0] = first
        edge_cols[1] = last
        edge_cols[2] = jnp.concatenate([mass] * (rows // 8), axis=0)

    def forward(m):
        ueast[m] = crecv[0, m, 1] + horiz_ratio * csend[0, m, 0]
        vnorth[m] = rrecv[0, m, 1] + horiz_ratio * rsend[0, m, 0]

        def level(k, dsum):
            pk = p[m, k]
            pw = jnp.where(lane == 0, pltpu.roll(crecv[0, m, 0], k + 1, 1), pltpu.roll(pk, 1, 1))
            ps = jnp.where(row == 0, rrecv[0, m, 0, pl.ds(k, 1), :], pltpu.roll(pk, 1, 0))
            uk = u[m, k] - horiz_ratio * (pk - pw)
            vk = v[m, k] - horiz_ratio * (pk - ps)
            ue = jnp.where(lane == cols - 1, pltpu.roll(ueast[m], k, 1), pltpu.roll(uk, cols - 1, 1))
            vn = jnp.where(row == rows - 1, vnorth[m, pl.ds(k, 1), :], pltpu.roll(vk, rows - 1, 0))
            div = (ue - uk) + (vn - vk)
            part = pk - horiz_ratio * s[k] * div
            p[m, k] = part
            return part, dsum + sig[k] * div

        def one(i, c):
            k = i + 1
            part_below, value = c[:2]
            part, dsum = level(k, c[2])
            rhs = w[m, i] - vert_ratio * (part - part_below)
            value = (rhs + (vert_ratio * vert_ratio) * s[i] * value) * inv[k]
            w[m, i] = value
            return part, value, dsum

        part, dsum = level(0, zero)
        return unrolled(levels - 1, one, (part, zero, dsum))[2]

    def backward(m):
        def finish(k, pk, last, first):
            p[m, k] = pk
            rsend[1, m, 0, pl.ds(k, 1), :] = pk[rows - 1 : rows, :]
            rsend[1, m, 1, pl.ds(k, 1), :] = pk[0:1, :]
            return pack_last(k, pk, last), pack_first(k, pk, first)

        def one(i, c):
            k = levels - 1 - i
            above = c[0]
            here = w[m, k - 1] + g[k] * above
            w[m, k - 1] = here
            pk = p[m, k] - vert_ratio * s[k] * (above - here)
            return (here,) + finish(k, pk, c[1], c[2])

        c = unrolled(levels - 1, one, (zero,) * 3)
        last, first = finish(0, p[m, 0] - vert_ratio * s[0] * c[0], c[1], c[2])
        csend[1, m, 0] = last
        csend[1, m, 1] = first

    def weigh(m):
        def level(k, mass, total):
            pk = p[m, k]
            around = (pltpu.roll(pk, 1, 1) + pltpu.roll(pk, cols - 1, 1)) + (
                pltpu.roll(pk, 1, 0) + pltpu.roll(pk, rows - 1, 0))
            return mass + thick[k] * pk, total + (alpha[k] * pk + sig[k] * around)

        def one(i, c):
            mass, total = level(i + 1, *c)
            return mass, total + lam[i + 1] * w[m, i]

        return unrolled(levels - 1, one, level(0, zero, zero))

    def integrals(m, usum, vsum, mass_before, dsum, mass, total):
        across = lambda x: jnp.sum(x, axis=1, keepdims=True)
        along = lambda x: jnp.sum(x, axis=0, keepdims=True)
        pw, ps = crecv[1, m, 0], rrecv[1, m, 0]
        total = total - dsum / horiz_ratio
        total = total + jnp.where(lane == 0, across(edge_cols[0] * (pw - csend[1, m, 0])), 0.0)
        total = total + jnp.where(
            lane == cols - 1, across(edge_cols[1] * (crecv[1, m, 1] - csend[1, m, 1])), 0.0)
        total = total + jnp.where(row == 0, along(edge_rows[0] * (ps - rsend[1, m, 0])), 0.0)
        total = total + jnp.where(
            row == rows - 1, along(edge_rows[1] * (rrecv[1, m, 1] - rsend[1, m, 1])), 0.0)
        mass, pw, ps = mass_before + mass, crecv[0, m, 0] + pw, rrecv[0, m, 0] + ps
        mass_west = jnp.where(lane == 0, across(edge_cols[2] * pw), pltpu.roll(mass, 1, 1))
        mass_south = jnp.where(row == 0, along(edge_rows[2] * ps), pltpu.roll(mass, 1, 0))
        return (
            total,
            usum - horiz_ratio * (mass - mass_west),
            vsum - horiz_ratio * (mass - mass_south),
        )

    sent = []

    def send_halos(sub, m):
        for copy in halo_copies(sub, m):
            copy.start()
            sent.append(copy)

    loads["s"].wait()
    pivots()
    raw = []
    for m in range(own):
        for name in "puv":
            loads[name, m].wait()
        raw.append(pack_inputs(m))
        if m == 0:
            pl.semaphore_wait(barrier, tiles - 1 + n_mem - 1)
        send_halos(0, m)

    sums = []
    for m in range(own):
        loads["w", m].wait()
        for copy in halo_copies(0, m):
            copy.wait_recv()
        sums.append((*raw[m], forward(m)))
        backward(m)
        send_halos(1, m)
    sums = [(*sums[m], *weigh(m)) for m in range(own)]
    for m in range(own):
        for copy in halo_copies(1, m):
            copy.wait_recv()
        for f, total in enumerate(integrals(m, *sums[m])):
            for q in range(n_mem):
                integ[m, q, f] = total[q * quarter : (q + 1) * quarter]
        for i in range(1, n_mem):
            other, where = mem_id(i)
            copy = remote(
                integ.at[m, other], gath.at[mem, m], ms_sem.at[m, other], mr_sem.at[m, mem], where)
            copy.start()
            sent.append(copy)

    fields = [[integ[m, mem, f] for f in range(3)] for m in range(own)]
    for m in range(own):
        for i in range(1, n_mem):
            other, where = mem_id(i)
            remote(integ.at[m, other], gath.at[other, m], ms_sem.at[m, other], mr_sem.at[m, other], where).wait_recv()
            fields.append([gath[other, m, f] for f in range(3)])
    members = len(fields)
    for f in range(3):
        total = fields[0][f]
        for one in fields[1:]:
            total = total + one[f]
        mean = total / members
        second = (fields[0][f] - mean) ** 2
        for one in fields[1:]:
            second = second + (one[f] - mean) ** 2
        everyone[me, f] = mean
        everyone[me, 3 + f] = second / (members - 1)

    for i in range(1, tiles):
        other, where = tile_id(i)
        copy = remote(everyone.at[me], everyone.at[me], as_sem.at[i], ar_sem.at[me], where)
        copy.start()
        sent.append(copy)
    mine = jnp.int32(0)
    for t in range(tiles):
        mine = jnp.where(owner[t] == me, t, mine)
    for i in range(1, tiles):
        other, where = tile_id(i)
        remote(everyone.at[me], everyone.at[other], as_sem.at[i], ar_sem.at[other], where).wait_recv()
    out[0, 0] = everyone[mine]
    for copy in sent:
        copy.wait_send()


def solution(mesh):
    n_mem, n_ty, n_tx = (mesh.shape[a] for a in ("mem", "ty", "tx"))
    tiles = n_ty * n_tx

    def local(pressure, east_wind, north_wind, vertical_wind, sound_squared, thickness, owner_map):
        own, levels, rows, cols = pressure.shape
        quarter = rows // n_mem
        f32 = jnp.float32
        dma = pltpu.SemaphoreType.DMA
        anywhere = pl.BlockSpec(memory_space=pl.ANY)
        scalars = pl.BlockSpec(memory_space=pltpu.SMEM)
        return pl.pallas_call(
            functools.partial(kernel, (n_mem, n_ty, n_tx)),
            name="acoustic",
            out_shape=jax.ShapeDtypeStruct((1, 1, 6, quarter, cols), f32),
            in_specs=[anywhere] * 5 + [scalars] * 2,
            out_specs=pl.BlockSpec(memory_space=pltpu.VMEM),
            scratch_shapes=[
                pltpu.VMEM((own, levels, rows, cols), f32),
                pltpu.VMEM((own, levels, rows, cols), f32),
                pltpu.VMEM((own, levels, rows, cols), f32),
                pltpu.VMEM((own, levels - 1, rows, cols), f32),
                *[pltpu.VMEM((levels, rows, cols), f32)] * 6,
                pltpu.VMEM((3, rows, cols), f32),
                pltpu.VMEM((3, levels, cols), f32),
                pltpu.VMEM((SUBSTEPS, own, 2, rows, cols), f32),
                pltpu.VMEM((SUBSTEPS, own, 2, rows, cols), f32),
                pltpu.VMEM((SUBSTEPS, own, 2, levels, cols), f32),
                pltpu.VMEM((SUBSTEPS, own, 2, levels, cols), f32),
                pltpu.VMEM((own, rows, cols), f32),
                pltpu.VMEM((own, levels, cols), f32),
                pltpu.VMEM((own, n_mem, 3, quarter, cols), f32),
                pltpu.VMEM((n_mem, own, 3, quarter, cols), f32),
                pltpu.VMEM((tiles, 6, quarter, cols), f32),
                dma((4 * own + 1,)),
                dma((SUBSTEPS, own, 2)),
                dma((SUBSTEPS, own, 2)),
                dma((SUBSTEPS, own, 2)),
                dma((SUBSTEPS, own, 2)),
                dma((own, n_mem)),
                dma((own, n_mem)),
                dma((tiles,)),
                dma((tiles,)),
            ],
            compiler_params=pltpu.CompilerParams(collective_id=0, has_side_effects=True),
        )(pressure, east_wind, north_wind, vertical_wind, sound_squared, thickness, owner_map)

    field = P("mem", None, "ty", "tx")
    return jax.shard_map(
        local,
        mesh=mesh,
        in_specs=(field, field, field, field, P(None, "ty", "tx"), P(), P()),
        out_specs=P("ty", "tx", None, "mem", None),
        check_vma=False,
    )
```
